128 devices in a mesh: lat: 8 (over x, core), lon: 16 (over z, y).
Axes of the slice: x: 4, y: 4, z: 4, core: 2. Of those that a mesh axis runs over, the one named last changes fastest.
Arguments:
- mesh_nodes: bfloat16 [32768, 512], P(('lat', 'lon')), may hold values from -6 to 6
- mesh_edges: bfloat16 [262144, 512], P(('lat', 'lon')), may hold values from -6 to 6
- grid_state: bfloat16 [256, 512, 512], P('lat', 'lon'), may hold values from -6 to 6
- decoder_edges: bfloat16 [3, 256, 512, 512], P(None, 'lat', 'lon'), may hold values from -6 to 6
- edge_send: int32 [262144], P(('lat', 'lon')), may hold values from 0 to 1279
- edge_recv: int32 [262144], P(('lat', 'lon')), may hold values from -1 to 255, as said below
- halo_lists: int32 [128, 128, 8], P(('lat', 'lon')), may hold values from 0 to 255
- decoder_lists: int32 [128, 128, 4], P(('lat', 'lon')), may hold values from 0 to 255
- decoder_sources: int32 [3, 256, 512], P(None, 'lat', 'lon'), may hold values from 0 to 511
- edge_first: bfloat16 [2, 1536, 512], replicated, may hold values from -0.15625 to 0.15625
- edge_second: bfloat16 [2, 512, 512], replicated, may hold values from -0.25 to 0.25
- node_first: bfloat16 [2, 1024, 512], replicated, may hold values from -0.1875 to 0.1875
- node_second: bfloat16 [2, 512, 512], replicated, may hold values from -0.25 to 0.25
- decoder_first: bfloat16 [1536, 512], replicated, may hold values from -0.15625 to 0.15625
- decoder_second: bfloat16 [512, 512], replicated, may hold values from -0.25 to 0.25
- grid_first: bfloat16 [1024, 512], replicated, may hold values from -0.1875 to 0.1875
- grid_second: bfloat16 [512, 512], replicated, may hold values from -0.25 to 0.25
Outputs:
- mesh_final: bfloat16 [32768, 512], P(('lat', 'lon'))
- grid_final: bfloat16 [256, 512, 512], P('lat', 'lon')
The draws below stay inside these ranges and needn't reach their ends.
Inputs may be any that keep to these rules, and one draw needn't show every extreme that they name: `edge_recv`: on each partition the live edges come first; their number is a multiple of 128, at least 128 and at most 2048, and some partition has 2048; live receivers are local node rows, padding slots hold -1.
All inputs are finite; a program needn't handle non-finite values.
Results may differ from the reference program's by a relative error of at most 0.012.
Values may be sent and summed in bfloat16 or wider, within the bound.
No kernel may reach another device: no remote copies, remote signals or barrier semaphores. Data moves between devices by JAX's collectives and lax.ppermute only.
A program may use at most 128 MiB of HBM per device.

```python
import jax
import jax.numpy as jnp
from jax import lax

W = 512
LAYERS = 2
M_DEV = 256
E_DEV = 2048
SLOTS = 8
DSLOTS = 4
TLAT = 32
TLON = 32
NODES = 32768
EDGES = 262144
LAT_ROWS = 256
LON_COLS = 512
N_LAT = 8
N_LON = 16
DEVICES = 128


def draw_edge_recv(key, part):
    block_count = E_DEV // 128
    key_blocks = jax.random.fold_in(key, 11)
    key_full = jax.random.fold_in(key, 23)
    key_rows = jax.random.fold_in(key, 37)
    raw_blocks = jax.random.randint(key_blocks, (DEVICES,), 0, block_count + 1)
    live_blocks = 1 + raw_blocks * raw_blocks // (block_count + 1)
    busiest = jax.random.randint(key_full, (), 0, DEVICES)
    live_blocks = jnp.where(jnp.arange(DEVICES) == busiest, block_count, live_blocks)
    receivers = jax.random.randint(key_rows, (DEVICES, E_DEV), 0, M_DEV)
    position = jnp.arange(E_DEV)
    chosen = jnp.where(position[None, :] < live_blocks[:, None] * 128, receivers, -1)
    return chosen.reshape(DEVICES * E_DEV).astype(jnp.int32)


def with_ends(values, stream_key, low, high):
    spot = [jax.random.randint(jax.random.fold_in(stream_key, axis), (), 0, length) for axis, length in enumerate(values.shape)]
    main_axis = values.shape.index(max(values.shape))
    next_to = spot[:main_axis] + [(spot[main_axis] + 1) % values.shape[main_axis]] + spot[main_axis + 1:]
    return values.at[tuple(spot)].set(low).at[tuple(next_to)].set(high)


def shard_levels(rng, shape, pieces, low, largest):
    loudness = 1.0
    for axis_at, shards_of in pieces:
        draws = jax.random.uniform(jax.random.fold_in(jax.random.fold_in(rng, 6), axis_at), (shards_of,), jnp.float32, low / len(pieces), largest / len(pieces))
        loudness = loudness * jnp.repeat(jnp.exp(draws), shape[axis_at] // shards_of).reshape((-1,) + (1,) * (len(shape) - 1 - axis_at))
    return loudness


def gaussian(stream_key, shape, deviation, limit, shards=(), held_as=jnp.bfloat16):
    gain = shard_levels(stream_key, shape, shards, -0.22, 0.18) if shards else 1.0
    values = jax.random.normal(stream_key, shape, jnp.float32) * deviation * gain
    return jnp.minimum(jnp.maximum(values, -limit), limit).astype(held_as)


def setup_inputs(seed: int = 0) -> dict:
    key_of = jax.random.split(jax.random.key(seed), 18)
    mesh_nodes = gaussian(key_of[0], (NODES, W), 1.0, 6.0, ((0, 128),))
    mesh_edges = gaussian(key_of[1], (EDGES, W), 1.0, 6.0, ((0, 128),))
    grid_state = gaussian(key_of[2], (LAT_ROWS, LON_COLS, W), 1.0, 6.0, ((0, 8), (1, 16)))
    decoder_edges = gaussian(key_of[3], (3, LAT_ROWS, LON_COLS, W), 1.0, 6.0, ((1, 8), (2, 16)))
    edge_send = with_ends(jax.random.randint(key_of[4], (EDGES,), 0, M_DEV + DEVICES * SLOTS), jax.random.fold_in(key_of[4], 1), 0, (M_DEV + DEVICES * SLOTS) - 1).astype(jnp.int32)
    edge_recv = draw_edge_recv(jax.random.fold_in(key_of[17], 71), 0)
    halo_lists = with_ends(jax.random.randint(key_of[6], (DEVICES, DEVICES, SLOTS), 0, M_DEV), jax.random.fold_in(key_of[6], 1), 0, M_DEV - 1).astype(jnp.int32)
    decoder_lists = with_ends(jax.random.randint(key_of[7], (DEVICES, DEVICES, DSLOTS), 0, M_DEV), jax.random.fold_in(key_of[7], 1), 0, M_DEV - 1).astype(jnp.int32)
    decoder_sources = with_ends(jax.random.randint(key_of[8], (3, LAT_ROWS, LON_COLS), 0, DEVICES * DSLOTS), jax.random.fold_in(key_of[8], 1), 0, (DEVICES * DSLOTS) - 1).astype(jnp.int32)
    edge_first = gaussian(key_of[9], (LAYERS, 3 * W, W), (3 * W) ** -0.5, 0.15625)
    edge_second = gaussian(key_of[10], (LAYERS, W, W), W ** -0.5, 0.25)
    node_first = gaussian(key_of[11], (LAYERS, 2 * W, W), (2 * W) ** -0.5, 0.1875)
    node_second = gaussian(key_of[12], (LAYERS, W, W), W ** -0.5, 0.25)
    decoder_first = gaussian(key_of[13], (3 * W, W), (3 * W) ** -0.5, 0.15625)
    decoder_second = gaussian(key_of[14], (W, W), W ** -0.5, 0.25)
    grid_first = gaussian(key_of[15], (2 * W, W), (2 * W) ** -0.5, 0.1875)
    grid_second = gaussian(key_of[16], (W, W), W ** -0.5, 0.25)
    return dict(mesh_nodes=mesh_nodes, mesh_edges=mesh_edges, grid_state=grid_state, decoder_edges=decoder_edges, edge_send=edge_send, edge_recv=edge_recv, halo_lists=halo_lists, decoder_lists=decoder_lists, decoder_sources=decoder_sources, edge_first=edge_first, edge_second=edge_second, node_first=node_first, node_second=node_second, decoder_first=decoder_first, decoder_second=decoder_second, grid_first=grid_first, grid_second=grid_second)


epsilon = 1e-05

def normalize(values):
    average = lax.optimization_barrier(jnp.mean(values, axis=-1, keepdims=True))
    centered = values - average
    spread = lax.optimization_barrier(jnp.mean(centered * centered, axis=-1, keepdims=True))
    return centered * lax.rsqrt(spread + epsilon)

def perceptron(inputs, layer_one, layer_two):
    hidden = jax.nn.silu(jnp.dot(inputs, layer_one, preferred_element_type=jnp.float32)).astype(jnp.bfloat16)
    return normalize(jnp.dot(hidden, layer_two, preferred_element_type=jnp.float32))

def mesh_layer(nodes_now, edges_now, edge_send, edge_recv, halo_lists, w_edge1, w_edge2, w_node1, w_node2):
    feature_width = nodes_now.shape[1]
    node_blocks = nodes_now.reshape(DEVICES, M_DEV, feature_width)
    edge_blocks = edges_now.reshape(DEVICES, E_DEV, feature_width)
    send_blocks = edge_send.reshape(DEVICES, E_DEV)
    recv_blocks = edge_recv.reshape(DEVICES, E_DEV)

    def one_part(device):
        own_rows = node_blocks[device]
        chosen = halo_lists[:, device, :]
        remote = jnp.take_along_axis(node_blocks, chosen[:, :, None], axis=1).reshape(DEVICES * SLOTS, feature_width)
        lookup = jnp.concatenate([own_rows, remote], axis=0)
        senders = jnp.take(lookup, send_blocks[device], axis=0)
        targets = recv_blocks[device]
        receivers = jnp.take(own_rows, jnp.maximum(targets, 0), axis=0)
        edge_rows = edge_blocks[device]
        inputs = jnp.concatenate([edge_rows, senders, receivers], axis=1)
        result = perceptron(inputs, w_edge1, w_edge2)
        message = lax.optimization_barrier(result.astype(jnp.bfloat16)).astype(jnp.float32)
        fresh = (edge_rows.astype(jnp.float32) + result).astype(jnp.bfloat16)
        segment = jnp.where(targets >= 0, targets, M_DEV).astype(jnp.int32)
        summed = jax.ops.segment_sum(message, segment, num_segments=M_DEV + 1)[:M_DEV]
        return (fresh, summed.astype(jnp.bfloat16))
    fresh_edges, gathered = lax.map(one_part, jnp.arange(DEVICES, dtype=jnp.int32))
    gathered = gathered.reshape(NODES, feature_width)
    inputs = jnp.concatenate([nodes_now, gathered], axis=1)
    result = perceptron(inputs, w_node1, w_node2)
    fresh_nodes = (nodes_now.astype(jnp.float32) + result).astype(jnp.bfloat16)
    return (fresh_nodes, fresh_edges.reshape(EDGES, feature_width))

def reference(mesh_nodes, mesh_edges, grid_state, decoder_edges, edge_send, edge_recv, halo_lists, decoder_lists, decoder_sources, edge_first, edge_second, node_first, node_second, decoder_first, decoder_second, grid_first, grid_second):
    nodes_now, edges_now = (mesh_nodes, mesh_edges)
    for layer in range(LAYERS):
        nodes_now, edges_now = mesh_layer(nodes_now, edges_now, edge_send, edge_recv, halo_lists, edge_first[layer], edge_second[layer], node_first[layer], node_second[layer])
    feature_width = nodes_now.shape[1]
    cells = TLAT * TLON
    node_blocks = nodes_now.reshape(DEVICES, M_DEV, feature_width)
    tiles = grid_state.reshape(N_LAT, TLAT, N_LON, TLON, feature_width).transpose(0, 2, 1, 3, 4).reshape(DEVICES, cells, feature_width)
    edge_tiles = decoder_edges.reshape(3, N_LAT, TLAT, N_LON, TLON, feature_width).transpose(1, 3, 0, 2, 4, 5).reshape(DEVICES, 3, cells, feature_width)
    source_tiles = decoder_sources.reshape(3, N_LAT, TLAT, N_LON, TLON).transpose(1, 3, 0, 2, 4).reshape(DEVICES, 3, cells)

    def one_tile(device):
        chosen = decoder_lists[:, device, :]
        lookup = jnp.take_along_axis(node_blocks, chosen[:, :, None], axis=1).reshape(DEVICES * DSLOTS, feature_width)
        grid_tile = tiles[device]
        summed = jnp.zeros((cells, feature_width), jnp.float32)
        for branch in range(3):
            mesh_rows = jnp.take(lookup, source_tiles[device, branch], axis=0)
            inputs = jnp.concatenate([edge_tiles[device, branch], mesh_rows, grid_tile], axis=1)
            result = perceptron(inputs, decoder_first, decoder_second)
            summed = summed + lax.optimization_barrier(result.astype(jnp.bfloat16)).astype(jnp.float32)
        gathered = summed.astype(jnp.bfloat16)
        result = perceptron(jnp.concatenate([grid_tile, gathered], axis=1), grid_first, grid_second)
        return (grid_tile.astype(jnp.float32) + result).astype(jnp.bfloat16)
    decoded = lax.map(one_tile, jnp.arange(DEVICES, dtype=jnp.int32))
    grid_final = decoded.reshape(N_LAT, N_LON, TLAT, TLON, feature_width).transpose(0, 2, 1, 3, 4).reshape(TLAT * N_LAT, TLON * N_LON, feature_width)
    return (nodes_now, grid_final)
```

```python
import functools

import jax
import jax.numpy as jnp
from jax import lax
from jax.experimental import pallas as pl
from jax.experimental.pallas import tpu as pltpu
from jax.sharding import PartitionSpec as P

epsilon = 1e-05
BLOCK = 512
CELLS = 256
GRANT = 62 << 20
bf16 = jnp.bfloat16
f32 = jnp.float32
HBM = pltpu.HBM
VMEM = pltpu.VMEM


def dot(a, b):
    return jnp.dot(a, b, preferred_element_type=f32)


def silu(values):
    half = values * 0.5
    return half + half * jnp.tanh(half)


def normalize(values):
    average = jnp.mean(values, axis=-1, keepdims=True)
    centered = values - average
    spread = jnp.mean(centered * centered, axis=-1, keepdims=True)
    return centered * lax.rsqrt(spread + epsilon)


def tail(before, second):
    return normalize(dot(silu(before).astype(bf16), second))


def picker_rows(row, table_rows, first):
    spread = jnp.broadcast_to(row.astype(f32), (128, 128)).T
    lanes = lax.broadcasted_iota(jnp.int32, (128, 128), 1).astype(f32)
    shifted = spread - lanes
    pieces = [
        jnp.where(shifted == float(first + c * 128), 1.0, 0.0).astype(bf16)
        for c in range(table_rows // 128)
    ]
    return jnp.concatenate(pieces, axis=1)


def fill_picker(oh_ref, idx_ref, first_index_row, rows, table_rows, first):
    for r in range(rows // 128):
        row = idx_ref[pl.ds(first_index_row + r, 1), :]
        oh_ref[r * 128 : (r + 1) * 128, :] = picker_rows(row, table_rows, first)


def pick_kernel(lists, nodes, out, oh):
    fill_picker(oh, lists, 0, out.shape[0], nodes.shape[0], 0)
    out[...] = dot(oh[...], nodes[...]).astype(bf16)


def pick_first(lists, nodes):
    rows = lists.shape[0] * 128
    return pl.pallas_call(
        pick_kernel,
        out_shape=jax.ShapeDtypeStruct((rows, nodes.shape[1]), bf16),
        in_specs=[pl.BlockSpec(memory_space=VMEM)] * 2,
        out_specs=pl.BlockSpec(memory_space=VMEM),
        scratch_shapes=[VMEM((rows, nodes.shape[0]), bf16)],
        compiler_params=pltpu.CompilerParams(vmem_limit_bytes=GRANT),
        cost_estimate=pl.CostEstimate(
            flops=2 * rows * nodes.shape[0] * nodes.shape[1], bytes_accessed=1 << 20, transcendentals=0
        ),
        name="pick_first",
    )(lists, nodes)


def before_kernel(live, edges, send, recv, nodes, first, out, oh):
    block = pl.program_id(0)
    width = nodes.shape[1]
    count = nodes.shape[0]

    @pl.when(block < live[0])
    def _():
        rows = edges.shape[0]
        steps = rows // 128
        fill_picker(oh, send, block * steps, rows, count, 0)
        from_send = dot(oh[...], nodes[...]).astype(bf16)
        total = dot(edges[...], first[0, :width, :]) + dot(from_send, first[0, width : 2 * width, :])
        fill_picker(oh, recv, block * steps, rows, count, 0)
        from_recv = dot(oh[...], nodes[...]).astype(bf16)
        out[...] = total + dot(from_recv, first[0, 2 * width :, :])


def edges_before(live, edges, send, recv, nodes, edge_first, layer):
    count, width = edges.shape
    blocks = count // BLOCK
    clamp = lambda i, live: (jnp.minimum(i, live[0] - 1), 0)
    whole = lambda i, live: (0, 0)
    grid_spec = pltpu.PrefetchScalarGridSpec(
        num_scalar_prefetch=1,
        grid=(blocks,),
        in_specs=[
            pl.BlockSpec((BLOCK, width), clamp),
            pl.BlockSpec(send.shape, whole),
            pl.BlockSpec(recv.shape, whole),
            pl.BlockSpec(nodes.shape, whole),
            pl.BlockSpec((1, 3 * width, width), lambda i, live: (layer, 0, 0)),
        ],
        out_specs=pl.BlockSpec((BLOCK, width), clamp),
        scratch_shapes=[VMEM((BLOCK, nodes.shape[0]), bf16)],
    )
    return pl.pallas_call(
        before_kernel,
        grid_spec=grid_spec,
        out_shape=jax.ShapeDtypeStruct((count, width), f32),
        compiler_params=pltpu.CompilerParams(vmem_limit_bytes=GRANT),
        cost_estimate=pl.CostEstimate(flops=8 * count * width * width, bytes_accessed=8 << 20, transcendentals=0),
        name=f"edges_before_{layer}",
    )(live, edges, send, recv, nodes, edge_first)


def layer_kernel(
    layer,
    last,
    live,
    send,
    recv_rows,
    lists,
    incoming,
    before,
    edges,
    nodes,
    edge_first,
    edge_second,
    node_first,
    node_second,
    *rest,
):
    if last:
        nodes_out, outgoing = rest[:2]
        rest = rest[2:]
        fresh_out = fresh = out_sem = edge_buf = None
    else:
        nodes_out, outgoing, fresh_out = rest[:3]
        rest = rest[3:]
        edge_buf, fresh, out_sem = rest[:3]
        rest = rest[3:]
    send_buf, before_buf, second_buf, node_buf, nf_buf, ns_buf, table, oh, oh_lists, acc, sem, bsem = rest
    width = nodes.shape[1]
    count = nodes.shape[0]
    blocks = before.shape[0] // BLOCK
    live_blocks = live[0]

    def copy(src, dst, which):
        return pltpu.make_async_copy(src, dst, sem.at[which])

    c_send = copy(edge_first.at[layer, pl.ds(width, width), :], send_buf, 1)
    c_second = copy(edge_second.at[layer], second_buf, 2)
    c_node = copy(nodes, node_buf, 3)
    c_nf = copy(node_first.at[layer], nf_buf, 4)
    c_ns = copy(node_second.at[layer], ns_buf, 5)

    def c_before(b):
        return pltpu.make_async_copy(
            before.at[pl.ds(b * BLOCK, BLOCK), :], before_buf.at[pl.ds(b * BLOCK, BLOCK), :], bsem.at[0, b]
        )

    def c_edge(b):
        return pltpu.make_async_copy(
            edges.at[pl.ds(b * BLOCK, BLOCK), :], edge_buf.at[pl.ds(b * BLOCK, BLOCK), :], bsem.at[1, b]
        )

    def c_fresh(b):
        return pltpu.make_async_copy(
            fresh.at[pl.ds(b * BLOCK, BLOCK), :], fresh_out.at[pl.ds(b * BLOCK, BLOCK), :], out_sem.at[b]
        )

    c_send.start()
    c_second.start()
    for b in range(blocks):

        @pl.when(b < live_blocks)
        def _(b=b):
            c_before(b).start()
            if not last:
                c_edge(b).start()

    c_node.start()
    c_nf.start()
    c_ns.start()
    acc[...] = jnp.zeros_like(acc)
    fill_picker(oh_lists, lists, 0, oh_lists.shape[0], count, 0)
    c_send.wait()
    table[...] = dot(incoming[...], send_buf[...]).astype(bf16)
    c_second.wait()

    def advance(b, carry):
        fill_picker(oh, send, b * (BLOCK // 128), BLOCK, table.shape[0], count)
        c_before(b).wait()
        rows = pl.ds(pl.multiple_of(b * BLOCK, BLOCK), BLOCK)
        result = tail(dot(oh[...], table[...]) + before_buf[rows, :], second_buf[...])
        target = recv_rows[pl.ds(b, 1), :]
        scatter = jnp.where(
            lax.broadcasted_iota(jnp.int32, (count, BLOCK), 0) == jnp.broadcast_to(target, (count, BLOCK)), 1.0, 0.0
        ).astype(bf16)
        acc[...] += dot(scatter, result.astype(bf16))
        if not last:
            c_edge(b).wait()
            fresh[rows, :] = (edge_buf[rows, :].astype(f32) + result).astype(bf16)
            c_fresh(b).start()
        return carry

    lax.fori_loop(0, live_blocks, advance, 0)
    c_node.wait()
    c_nf.wait()
    c_ns.wait()
    now = node_buf[...]
    before_node = dot(now, nf_buf[:width, :]) + dot(acc[...].astype(bf16), nf_buf[width:, :])
    updated = (now.astype(f32) + tail(before_node, ns_buf[...])).astype(bf16)
    nodes_out[...] = updated
    picked = dot(oh_lists[...], updated)
    if last:
        half = width // 2
        place = lax.broadcasted_iota(jnp.int32, (picked.shape[0], half), 0) % 8
        picked = jnp.where(place < 4, picked[:, :half], picked[:, half:])
    outgoing[...] = picked.astype(bf16)
    if not last:

        def drain(b, carry):
            c_fresh(b).wait()
            return carry

        lax.fori_loop(0, live_blocks, drain, 0)


def run_layer(layer, last, live, send, recv_rows, lists, incoming, before, edges, nodes, ef, es, nf, ns):
    count, width = nodes.shape
    edge_count = edges.shape[0]
    blocks = edge_count // BLOCK
    out_rows = lists.shape[0] * 128
    vm = pl.BlockSpec(memory_space=VMEM)
    hb = pl.BlockSpec(memory_space=HBM)
    out_shape = [
        jax.ShapeDtypeStruct((count, width), bf16),
        jax.ShapeDtypeStruct((out_rows, width // 2 if last else width), bf16),
    ]
    out_specs = [vm, vm]
    scratch = []
    if not last:
        out_shape.append(jax.ShapeDtypeStruct((edge_count, width), bf16))
        out_specs.append(hb)
        scratch += [VMEM((edge_count, width), bf16), VMEM((edge_count, width), bf16), pltpu.SemaphoreType.DMA((blocks,))]
    scratch += [
        VMEM((width, width), bf16),
        VMEM((edge_count, width), f32),
        VMEM((width, width), bf16),
        VMEM((count, width), bf16),
        VMEM((2 * width, width), bf16),
        VMEM((width, width), bf16),
        VMEM(incoming.shape, bf16),
        VMEM((BLOCK, incoming.shape[0]), bf16),
        VMEM((out_rows, count), bf16),
        VMEM((count, width), f32),
        pltpu.SemaphoreType.DMA((6,)),
        pltpu.SemaphoreType.DMA((2, blocks)),
    ]
    return pl.pallas_call(
        functools.partial(layer_kernel, layer, last),
        out_shape=out_shape,
        in_specs=[pl.BlockSpec(memory_space=pltpu.SMEM), vm, vm, vm, vm] + [hb] * 7,
        out_specs=out_specs,
        scratch_shapes=scratch,
        compiler_params=pltpu.CompilerParams(vmem_limit_bytes=GRANT),
        cost_estimate=pl.CostEstimate(flops=9 * edge_count * width * width, bytes_accessed=12 << 20, transcendentals=0),
        name=f"layer_{layer}",
    )(live, send, recv_rows, lists, incoming, before, edges, nodes, ef, es, nf, ns)


def decode_before_kernel(edges, grid, first, grid_first, out, out_grid):
    width = grid.shape[1]
    cells = grid.shape[0]
    out_grid[...] = dot(grid[...], grid_first[...])
    rows = edges[...].reshape(3 * cells, width)
    own = dot(rows, first[:width, :]).reshape(3, cells, width)
    out[...] = own + dot(grid[...], first[2 * width :, :])[None]


def decode_before(edges, grid, first, grid_first):
    cells, width = grid.shape
    whole = lambda i: (0, 0)
    return pl.pallas_call(
        decode_before_kernel,
        grid=(cells // CELLS,),
        in_specs=[
            pl.BlockSpec((3, CELLS, width), lambda i: (0, i, 0)),
            pl.BlockSpec((CELLS, width), lambda i: (i, 0)),
            pl.BlockSpec((3 * width, width), whole),
            pl.BlockSpec((width, width), whole),
        ],
        out_specs=[
            pl.BlockSpec((3, CELLS, width), lambda i: (0, i, 0)),
            pl.BlockSpec((CELLS, width), lambda i: (i, 0)),
        ],
        out_shape=[
            jax.ShapeDtypeStruct((3, cells, width), f32),
            jax.ShapeDtypeStruct((cells, width), f32),
        ],
        compiler_params=pltpu.CompilerParams(vmem_limit_bytes=GRANT),
        cost_estimate=pl.CostEstimate(flops=10 * cells * width * width, bytes_accessed=14 << 20, transcendentals=0),
        name="decode_before",
    )(edges, grid, first, grid_first)


def decode_kernel(
    sources, incoming, before, before_grid, grid, first, second, grid_first, grid_second, out,
    mid_buf, before_buf, bg_buf, grid_buf, second_buf, gf_buf, gs_buf, table, oh, out_buf, sem, bsem, osem,
):
    width = grid.shape[1]
    cells = grid.shape[0]
    blocks = cells // CELLS
    half = width // 2

    def copy(src, dst, which):
        return pltpu.make_async_copy(src, dst, sem.at[which])

    c_mid = copy(first.at[pl.ds(width, width), :], mid_buf, 1)
    c_second = copy(second, second_buf, 2)
    c_gf = copy(grid_first.at[pl.ds(width, width), :], gf_buf, 3)
    c_gs = copy(grid_second, gs_buf, 4)

    def c_before(b):
        rows = pl.ds(b * CELLS, CELLS)
        return pltpu.make_async_copy(before.at[:, rows, :], before_buf.at[:, rows, :], bsem.at[0, b])

    def c_bg(b):
        rows = pl.ds(b * CELLS, CELLS)
        return pltpu.make_async_copy(before_grid.at[rows, :], bg_buf.at[rows, :], bsem.at[1, b])

    def c_grid(b):
        rows = pl.ds(b * CELLS, CELLS)
        return pltpu.make_async_copy(grid.at[rows, :], grid_buf.at[rows, :], bsem.at[2, b])

    def c_out(b):
        rows = pl.ds(b * CELLS, CELLS)
        return pltpu.make_async_copy(out_buf.at[rows, :], out.at[rows, :], osem.at[b])

    c_mid.start()
    c_before(0).start()
    c_second.start()
    c_gf.start()
    c_gs.start()
    c_bg(0).start()
    c_grid(0).start()
    for b in range(1, blocks):
        c_before(b).start()
        c_bg(b).start()
        c_grid(b).start()
    packed = incoming[...].astype(f32).reshape(cells // 16, 16, half)
    even, odd = packed[:, :8, :], packed[:, 8:, :]
    low = lax.broadcasted_iota(jnp.int32, even.shape, 1) < 4
    left = jnp.where(low, even, pltpu.roll(odd, 4, 1))
    right = jnp.where(low, pltpu.roll(even, 4, 1), odd)
    left = left.reshape(cells // 2, half).astype(bf16)
    right = right.reshape(cells // 2, half).astype(bf16)
    c_mid.wait()
    table[...] = (dot(left, mid_buf[:half, :]) + dot(right, mid_buf[half:, :])).astype(bf16)
    c_second.wait()
    c_gf.wait()
    c_gs.wait()
    steps = CELLS // 128

    def advance(b, carry):
        rows = pl.ds(pl.multiple_of(b * CELLS, CELLS), CELLS)
        c_before(b).wait()
        summed = jnp.zeros((CELLS, width), f32)
        for branch in range(3):
            fill_picker(oh.at[branch], sources, branch * (cells // 128) + b * steps, CELLS, table.shape[0], 0)
            result = tail(dot(oh[branch], table[...]) + before_buf[branch, rows, :], second_buf[...])
            summed = summed + result.astype(bf16).astype(f32)
        c_bg(b).wait()
        c_grid(b).wait()
        result = tail(dot(summed.astype(bf16), gf_buf[...]) + bg_buf[rows, :], gs_buf[...])
        out_buf[rows, :] = (grid_buf[rows, :].astype(f32) + result).astype(bf16)
        c_out(b).start()
        return carry

    lax.fori_loop(0, blocks, advance, 0)

    def drain(b, carry):
        c_out(b).wait()
        return carry

    lax.fori_loop(0, blocks, drain, 0)


def decode(sources, incoming, before, before_grid, grid, first, second, grid_first, grid_second):
    cells, width = grid.shape
    blocks = cells // CELLS
    hb = pl.BlockSpec(memory_space=HBM)
    return pl.pallas_call(
        decode_kernel,
        out_shape=jax.ShapeDtypeStruct((cells, width), bf16),
        in_specs=[pl.BlockSpec(memory_space=VMEM)] * 2 + [hb] * 7,
        out_specs=hb,
        scratch_shapes=[
            VMEM((width, width), bf16),
            VMEM((3, cells, width), f32),
            VMEM((cells, width), f32),
            VMEM((cells, width), bf16),
            VMEM((width, width), bf16),
            VMEM((width, width), bf16),
            VMEM((width, width), bf16),
            VMEM((incoming.shape[0] // 2, width), bf16),
            VMEM((3, CELLS, incoming.shape[0] // 2), bf16),
            VMEM((cells, width), bf16),
            pltpu.SemaphoreType.DMA((5,)),
            pltpu.SemaphoreType.DMA((3, blocks)),
            pltpu.SemaphoreType.DMA((blocks,)),
        ],
        compiler_params=pltpu.CompilerParams(vmem_limit_bytes=GRANT),
        cost_estimate=pl.CostEstimate(flops=16 * cells * width * width, bytes_accessed=13 << 20, transcendentals=0),
        name="decode",
    )(sources, incoming, before, before_grid, grid, first, second, grid_first, grid_second)


def exchange(rows):
    chunks = rows.reshape(-1, 8, rows.shape[1])
    return lax.all_to_all(chunks, ("lat", "lon"), split_axis=0, concat_axis=0, tiled=True).reshape(rows.shape)


def shards(
    mesh_nodes,
    mesh_edges,
    grid_state,
    decoder_edges,
    edge_send,
    edge_recv,
    halo_lists,
    decoder_lists,
    decoder_sources,
    edge_first,
    edge_second,
    node_first,
    node_second,
    decoder_first,
    decoder_second,
    grid_first,
    grid_second,
):
    tile_lat, tile_lon, width = grid_state.shape
    cells = tile_lat * tile_lon
    halo = halo_lists.reshape(-1, 128)
    outgoing = pick_first(halo, mesh_nodes)
    incoming = exchange(outgoing)
    live = (jnp.sum((edge_recv >= 0).astype(jnp.int32)) + (BLOCK - 1)) // BLOCK
    live = live.reshape(1)
    send = edge_send.reshape(-1, 128)
    recv = edge_recv.reshape(-1, 128)
    recv_rows = edge_recv.reshape(-1, BLOCK)
    decoder_rows = decoder_lists.reshape(decoder_lists.shape[1], decoder_lists.shape[2])
    decoder_rows = jnp.concatenate([decoder_rows, decoder_rows], axis=1).reshape(-1, 128)
    grid = grid_state.reshape(cells, width)
    sources = decoder_sources.reshape(-1, 128)
    nodes, edges = mesh_nodes, mesh_edges
    layers = edge_first.shape[0]
    for layer in range(layers):
        last = layer == layers - 1
        before = edges_before(live, edges, send, recv, nodes, edge_first, layer)
        results = run_layer(
            layer, last, live, send, recv_rows, decoder_rows if last else halo, incoming, before, edges, nodes,
            edge_first, edge_second, node_first, node_second,
        )
        nodes, outgoing = results[:2]
        if not last:
            edges = results[2]
        incoming = exchange(outgoing)
    before, before_grid = decode_before(decoder_edges.reshape(3, cells, width), grid, decoder_first, grid_first)
    final = decode(
        sources, incoming, before, before_grid, grid, decoder_first, decoder_second, grid_first, grid_second
    )
    return nodes, final.reshape(tile_lat, tile_lon, width)


def solution(mesh):
    placed = (
        P(("lat", "lon"), None),
        P(("lat", "lon"), None),
        P("lat", "lon", None),
        P(None, "lat", "lon", None),
        P(("lat", "lon")),
        P(("lat", "lon")),
        P(("lat", "lon"), None, None),
        P(("lat", "lon"), None, None),
        P(None, "lat", "lon"),
        P(),
        P(),
        P(),
        P(),
        P(),
        P(),
        P(),
        P(),
    )
    return jax.shard_map(
        shards,
        mesh=mesh,
        in_specs=placed,
        out_specs=(P(("lat", "lon"), None), P("lat", "lon", None)),
        check_vma=False,
    )
```

```python
import functools

import jax
import jax.numpy as jnp
from jax import lax
from jax.experimental import pallas as pl
from jax.experimental.pallas import tpu as pltpu
from jax.sharding import PartitionSpec as P

epsilon = 1e-05
BLOCK = 512
SUB = 256
CHUNK = 32
CELLS = 256
GRANT = 40 << 20
bf16 = jnp.bfloat16
f32 = jnp.float32
HBM = pltpu.HBM
VMEM = pltpu.VMEM


def pinned(*arrays):
    return [pltpu.with_memory_space_constraint(a, HBM) for a in arrays]


def dot(a, b):
    return jnp.dot(a, b, preferred_element_type=f32)


def silu_of_double(half):
    return half + half * jnp.tanh(half)


def normalize(values):
    average = jnp.mean(values, axis=-1, keepdims=True)
    centered = values - average
    spread = jnp.mean(centered * centered, axis=-1, keepdims=True)
    return centered * lax.rsqrt(spread + epsilon)


def tail(half, second):
    return normalize(dot(silu_of_double(half).astype(bf16), second))


def picker_rows(row, table_rows, first):
    spread = jnp.broadcast_to(row.astype(f32), (128, 128)).T
    lanes = lax.broadcasted_iota(jnp.int32, (128, 128), 1).astype(f32)
    shifted = spread - lanes
    pieces = [
        jnp.where(shifted == float(first + c * 128), 1.0, 0.0).astype(bf16)
        for c in range(table_rows // 128)
    ]
    return jnp.concatenate(pieces, axis=1)


def fill_picker(oh_ref, idx_ref, first_index_row, rows, table_rows, first):
    for r in range(rows // 128):
        row = idx_ref[pl.ds(first_index_row + r, 1), :]
        oh_ref[r * 128 : (r + 1) * 128, :] = picker_rows(row, table_rows, first)


def fill_lists(oh_ref, lists_ref, spread_ref):
    slots = lists_ref.shape[0]
    for s in range(8):
        row = lists_ref[s % slots : s % slots + 1, :]
        spread_ref[pl.ds(s, 128, stride=8), :] = jnp.broadcast_to(row.astype(f32), (128, 128)).T
    lanes = lax.broadcasted_iota(jnp.int32, spread_ref.shape, 1).astype(f32)
    shifted = spread_ref[...] - lanes
    for c in range(oh_ref.shape[1] // 128):
        oh_ref[:, c * 128 : (c + 1) * 128] = jnp.where(shifted == float(c * 128), 1.0, 0.0).astype(bf16)


def pick_kernel(lists, nodes, out, oh, spread):
    fill_lists(oh, lists, spread)
    out[...] = dot(oh[...], nodes[...]).astype(bf16)


def pick_first(lists, nodes):
    rows = lists.shape[1] * 8
    return pl.pallas_call(
        pick_kernel,
        out_shape=jax.ShapeDtypeStruct((rows, nodes.shape[1]), bf16),
        in_specs=[pl.BlockSpec(memory_space=VMEM)] * 2,
        out_specs=pl.BlockSpec(memory_space=VMEM),
        scratch_shapes=[VMEM((rows, nodes.shape[0]), bf16), VMEM((rows, 128), f32)],
        compiler_params=pltpu.CompilerParams(vmem_limit_bytes=GRANT),
        cost_estimate=pl.CostEstimate(
            flops=2 * rows * nodes.shape[0] * nodes.shape[1], bytes_accessed=1 << 20, transcendentals=0
        ),
        name="pick_first",
    )(lists, nodes)


def before_kernel(edges, send, recv, nodes, first, out, oh):
    block = pl.program_id(0)
    width = nodes.shape[1]
    count = nodes.shape[0]

    rows = edges.shape[0]
    steps = rows // 128
    fill_picker(oh, send, block * steps, rows, count, 0)
    from_send = dot(oh[...], nodes[...]).astype(bf16)
    total = dot(edges[...], first[0, :width, :]) + dot(from_send, first[0, width : 2 * width, :])
    fill_picker(oh, recv, block * steps, rows, count, 0)
    from_recv = dot(oh[...], nodes[...]).astype(bf16)
    out[...] = (0.5 * (total + dot(from_recv, first[0, 2 * width :, :]))).astype(bf16)


def edges_before(edges, send, recv, nodes, edge_first, layer):
    count, width = edges.shape
    blocks = count // BLOCK
    clamp = lambda i: (i, 0)
    whole = lambda i: (0, 0)
    grid_spec = pl.GridSpec(
        grid=(blocks,),
        in_specs=[
            pl.BlockSpec((BLOCK, width), clamp),
            pl.BlockSpec(send.shape, whole),
            pl.BlockSpec(recv.shape, whole),
            pl.BlockSpec(nodes.shape, whole),
            pl.BlockSpec((1, 3 * width, width), lambda i: (layer, 0, 0)),
        ],
        out_specs=pl.BlockSpec((BLOCK, width), clamp),
        scratch_shapes=[VMEM((BLOCK, nodes.shape[0]), bf16)],
    )
    return pl.pallas_call(
        before_kernel,
        grid_spec=grid_spec,
        out_shape=jax.ShapeDtypeStruct((count, width), bf16),
        compiler_params=pltpu.CompilerParams(vmem_limit_bytes=GRANT),
        cost_estimate=pl.CostEstimate(flops=8 * count * width * width, bytes_accessed=8 << 20, transcendentals=0),
        name=f"edges_before_{layer}",
    )(edges, send, recv, nodes, edge_first)


def layer_kernel(
    layer,
    last,
    send,
    recv,
    lists,
    incoming,
    before,
    edges,
    nodes,
    edge_first,
    edge_second,
    node_first,
    node_second,
    *rest,
):
    if last:
        nodes_out, outgoing = rest[:2]
        rest = rest[2:]
        fresh_out = fresh = out_sem = edge_buf = None
    else:
        nodes_out, outgoing, fresh_out = rest[:3]
        rest = rest[3:]
        edge_buf, fresh, out_sem = rest[:3]
        rest = rest[3:]
    send_buf, before_buf, second_buf, node_buf, nf_buf, ns_buf, table, oh, ready, oh_lists, acc, spread, hidden, raw, message, scatter, sem, bsem = rest
    width = nodes.shape[1]
    count = nodes.shape[0]
    blocks = before.shape[0] // BLOCK

    def copy(src, dst, which):
        return pltpu.make_async_copy(src, dst, sem.at[which])

    c_send = copy(edge_first.at[layer, pl.ds(width, width), :], send_buf, 1)
    c_second = copy(edge_second.at[layer], second_buf, 2)
    c_node = copy(nodes, node_buf, 3)
    c_nf = copy(node_first.at[layer], nf_buf, 4)
    c_ns = copy(node_second.at[layer], ns_buf, 5)

    def c_before(b):
        return pltpu.make_async_copy(
            before.at[pl.ds(b * BLOCK, BLOCK), :], before_buf.at[pl.ds(b * BLOCK, BLOCK), :], bsem.at[0, b]
        )

    def c_edge(b):
        return pltpu.make_async_copy(
            edges.at[pl.ds(b * BLOCK, BLOCK), :], edge_buf.at[pl.ds(b * BLOCK, BLOCK), :], bsem.at[1, b]
        )

    def c_fresh(b):
        return pltpu.make_async_copy(
            fresh.at[pl.ds(b * BLOCK, BLOCK), :], fresh_out.at[pl.ds(b * BLOCK, BLOCK), :], out_sem.at[b]
        )

    c_send.start()
    c_before(0).start()
    c_second.start()
    for b in range(1, blocks):
        c_before(b).start()
    if not last:
        for b in range(blocks):
            c_edge(b).start()
    c_node.start()
    c_nf.start()
    c_ns.start()
    steps = SUB // 128
    items = before.shape[0] // SUB

    def picker(i):
        fill_picker(oh.at[i % 3], send, i * steps, SUB, table.shape[0], count)

    def first_half(i, part):
        columns = slice(part * (width // 2), (part + 1) * (width // 2))
        ready[i % 2, :, columns] = dot(oh[i % 3], table[:, columns])

    def hide(i):
        for c in range(0, SUB, CHUNK):
            half = ready[i % 2, c : c + CHUNK, :] + before_buf[i * SUB + c : i * SUB + c + CHUNK, :].astype(f32)
            hidden[c : c + CHUNK, :] = silu_of_double(half).astype(bf16)

    def finish(i):
        for r in range(steps):
            row = jnp.broadcast_to(recv[i * steps + r : i * steps + r + 1, :], (count, 128))
            hit = lax.broadcasted_iota(jnp.int32, (count, 128), 0) == row
            scatter[:, r * 128 : (r + 1) * 128] = jnp.where(hit, 1.0, 0.0).astype(bf16)
        for c in range(0, SUB, CHUNK):
            rows = slice(i * SUB + c, i * SUB + c + CHUNK)
            result = normalize(raw[c : c + CHUNK, :])
            message[c : c + CHUNK, :] = result.astype(bf16)
            if not last:
                fresh[rows, :] = (edge_buf[rows, :].astype(f32) + result).astype(bf16)
        part = dot(scatter[...], message[...])
        if i == 0:
            acc[...] = part
        else:
            acc[...] += part

    picker(0)
    picker(1)
    fill_lists(oh_lists, lists, spread)
    c_send.wait()
    table[...] = (0.5 * dot(incoming[...], send_buf[...])).astype(bf16)
    c_second.wait()
    per = BLOCK // SUB
    c_before(0).wait()
    first_half(0, 0)
    first_half(0, 1)
    for i in range(items):
        if i + 1 < items and (i + 1) % per == 0:
            c_before((i + 1) // per).wait()
        if not last and i % per == 0:
            c_edge(i // per).wait()
        if i + 2 < items:
            picker(i + 2)
        hide(i)
        if i + 1 < items:
            first_half(i + 1, 0)
        raw[...] = dot(hidden[...], second_buf[...])
        if i + 1 < items:
            first_half(i + 1, 1)
        finish(i)
        if not last and (i + 1) % (BLOCK // SUB) == 0:
            c_fresh(i // (BLOCK // SUB)).start()
    c_node.wait()
    c_nf.wait()
    c_ns.wait()
    now = node_buf[...]
    before_node = 0.5 * (dot(now, nf_buf[:width, :]) + dot(acc[...].astype(bf16), nf_buf[width:, :]))
    updated = (now.astype(f32) + tail(before_node, ns_buf[...])).astype(bf16)
    nodes_out[...] = updated
    picked = dot(oh_lists[...], updated)
    if last:
        half = width // 2
        place = lax.broadcasted_iota(jnp.int32, (picked.shape[0], half), 0) % 8
        picked = jnp.where(place < 4, picked[:, :half], picked[:, half:])
    outgoing[...] = picked.astype(bf16)
    if not last:
        for b in range(blocks):
            c_fresh(b).wait()


def run_layer(layer, last, send, recv, lists, incoming, before, edges, nodes, ef, es, nf, ns):
    count, width = nodes.shape
    edge_count = edges.shape[0]
    blocks = edge_count // BLOCK
    out_rows = lists.shape[1] * 8
    vm = pl.BlockSpec(memory_space=VMEM)
    hb = pl.BlockSpec(memory_space=HBM)
    out_shape = [
        jax.ShapeDtypeStruct((count, width), bf16),
        jax.ShapeDtypeStruct((out_rows, width // 2 if last else width), bf16),
    ]
    out_specs = [vm, vm]
    scratch = []
    if not last:
        out_shape.append(jax.ShapeDtypeStruct((edge_count, width), bf16))
        out_specs.append(hb)
        scratch += [VMEM((edge_count, width), bf16), VMEM((edge_count, width), bf16), pltpu.SemaphoreType.DMA((blocks,))]
    scratch += [
        VMEM((width, width), bf16),
        VMEM((edge_count, width), bf16),
        VMEM((width, width), bf16),
        VMEM((count, width), bf16),
        VMEM((2 * width, width), bf16),
        VMEM((width, width), bf16),
        VMEM(incoming.shape, bf16),
        VMEM((3, SUB, incoming.shape[0]), bf16),
        VMEM((2, SUB, width), f32),
        VMEM((out_rows, count), bf16),
        VMEM((count, width), f32),
        VMEM((out_rows, 128), f32),
        VMEM((SUB, width), bf16),
        VMEM((SUB, width), f32),
        VMEM((SUB, width), bf16),
        VMEM((count, SUB), bf16),
        pltpu.SemaphoreType.DMA((6,)),
        pltpu.SemaphoreType.DMA((2, blocks)),
    ]
    return pl.pallas_call(
        functools.partial(layer_kernel, layer, last),
        out_shape=out_shape,
        in_specs=[vm] * 4 + [hb] * 7,
        out_specs=out_specs,
        scratch_shapes=scratch,
        compiler_params=pltpu.CompilerParams(vmem_limit_bytes=GRANT),
        cost_estimate=pl.CostEstimate(flops=9 * edge_count * width * width, bytes_accessed=12 << 20, transcendentals=0),
        name=f"layer_{layer}",
    )(send, recv, lists, incoming, *pinned(before, edges, nodes, ef, es, nf, ns))


def decode_before_kernel(edges, grid, first, grid_first, out, out_grid):
    width = grid.shape[1]
    cells = grid.shape[0]
    out_grid[...] = (0.5 * dot(grid[...], grid_first[...])).astype(bf16)
    rows = edges[...].reshape(3 * cells, width)
    own = dot(rows, first[:width, :]).reshape(3, cells, width)
    out[...] = (0.5 * (own + dot(grid[...], first[2 * width :, :])[None])).astype(bf16)


def decode_before(edges, grid, first, grid_first):
    cells, width = grid.shape
    whole = lambda i: (0, 0)
    return pl.pallas_call(
        decode_before_kernel,
        grid=(cells // CELLS,),
        in_specs=[
            pl.BlockSpec((3, CELLS, width), lambda i: (0, i, 0)),
            pl.BlockSpec((CELLS, width), lambda i: (i, 0)),
            pl.BlockSpec((3 * width, width), whole),
            pl.BlockSpec((width, width), whole),
        ],
        out_specs=[
            pl.BlockSpec((3, CELLS, width), lambda i: (0, i, 0)),
            pl.BlockSpec((CELLS, width), lambda i: (i, 0)),
        ],
        out_shape=[
            jax.ShapeDtypeStruct((3, cells, width), bf16),
            jax.ShapeDtypeStruct((cells, width), bf16),
        ],
        compiler_params=pltpu.CompilerParams(vmem_limit_bytes=GRANT),
        cost_estimate=pl.CostEstimate(flops=10 * cells * width * width, bytes_accessed=14 << 20, transcendentals=0),
        name="decode_before",
    )(edges, grid, first, grid_first)


def decode_kernel(
    sources, incoming, before, before_grid, grid, first, second, grid_first, grid_second, out,
    mid_buf, before_buf, bg_buf, grid_buf, second_buf, gf_buf, gs_buf, table, oh, ready, summed, hidden, raw, ready_cells, hidden_cells, raw_cells, out_buf, sem, bsem, osem,
):
    width = grid.shape[1]
    cells = grid.shape[0]
    blocks = cells // CELLS
    half = width // 2

    def copy(src, dst, which):
        return pltpu.make_async_copy(src, dst, sem.at[which])

    c_mid = copy(first.at[pl.ds(width, width), :], mid_buf, 1)
    c_second = copy(second, second_buf, 2)
    c_gf = copy(grid_first.at[pl.ds(width, width), :], gf_buf, 3)
    c_gs = copy(grid_second, gs_buf, 4)

    def c_before(b):
        rows = pl.ds(b * CELLS, CELLS)
        return pltpu.make_async_copy(before.at[:, rows, :], before_buf.at[:, rows, :], bsem.at[0, b])

    def c_bg(b):
        rows = pl.ds(b * CELLS, CELLS)
        return pltpu.make_async_copy(before_grid.at[rows, :], bg_buf.at[rows, :], bsem.at[1, b])

    def c_grid(b):
        rows = pl.ds(b * CELLS, CELLS)
        return pltpu.make_async_copy(grid.at[rows, :], grid_buf.at[rows, :], bsem.at[2, b])

    def c_out(b):
        rows = pl.ds(b * CELLS, CELLS)
        return pltpu.make_async_copy(out_buf.at[rows, :], out.at[rows, :], osem.at[b])

    c_mid.start()
    c_before(0).start()
    c_second.start()
    c_gf.start()
    c_gs.start()
    c_bg(0).start()
    c_grid(0).start()
    for b in range(1, blocks):
        c_before(b).start()
        c_bg(b).start()
        c_grid(b).start()
    packed = incoming[...].astype(f32).reshape(cells // 16, 16, half)
    even, odd = packed[:, :8, :], packed[:, 8:, :]
    low = lax.broadcasted_iota(jnp.int32, even.shape, 1) < 4
    left = jnp.where(low, even, pltpu.roll(odd, 4, 1))
    right = jnp.where(low, pltpu.roll(even, 4, 1), odd)
    left = left.reshape(cells // 2, half).astype(bf16)
    right = right.reshape(cells // 2, half).astype(bf16)
    c_mid.wait()
    table[...] = (0.5 * (dot(left, mid_buf[:half, :]) + dot(right, mid_buf[half:, :]))).astype(bf16)
    c_second.wait()
    c_gf.wait()
    c_gs.wait()
    c_before(0).wait()
    steps = CELLS // 128
    items = [(b, branch) for b in range(blocks) for branch in range(3)]

    def picker(i):
        b, branch = items[i]
        fill_picker(oh.at[i % 3], sources, branch * (cells // 128) + b * steps, CELLS, table.shape[0], 0)

    def first_half(i, part):
        columns = slice(part * half, (part + 1) * half)
        ready[i % 2, :, columns] = dot(oh[i % 3], table[:, columns])

    def hide(i):
        b, branch = items[i]
        for c in range(0, CELLS, CHUNK):
            rows = slice(b * CELLS + c, b * CELLS + c + CHUNK)
            value = ready[i % 2, c : c + CHUNK, :] + before_buf[branch, rows, :].astype(f32)
            hidden[c : c + CHUNK, :] = silu_of_double(value).astype(bf16)

    def finish(i):
        branch = items[i][1]
        for c in range(0, CELLS, CHUNK):
            rows = slice(c, c + CHUNK)
            result = normalize(raw[rows, :]).astype(bf16).astype(f32)
            summed[rows, :] = result if branch == 0 else summed[rows, :] + result

    def finish_cells(b):
        c_bg(b).wait()
        c_grid(b).wait()
        ready_cells[...] = dot(summed[...].astype(bf16), gf_buf[...])
        for c in range(0, CELLS, CHUNK):
            rows = slice(b * CELLS + c, b * CELLS + c + CHUNK)
            value = 0.5 * ready_cells[c : c + CHUNK, :] + bg_buf[rows, :].astype(f32)
            hidden_cells[c : c + CHUNK, :] = silu_of_double(value).astype(bf16)
        raw_cells[...] = dot(hidden_cells[...], gs_buf[...])
        for c in range(0, CELLS, CHUNK):
            rows = slice(b * CELLS + c, b * CELLS + c + CHUNK)
            result = normalize(raw_cells[c : c + CHUNK, :])
            out_buf[rows, :] = (grid_buf[rows, :].astype(f32) + result).astype(bf16)
        c_out(b).start()

    picker(0)
    picker(1)
    first_half(0, 0)
    first_half(0, 1)
    for i, (b, branch) in enumerate(items):
        if branch == 2 and b + 1 < blocks:
            c_before(b + 1).wait()
        if i + 2 < len(items):
            picker(i + 2)
        hide(i)
        if i + 1 < len(items):
            first_half(i + 1, 0)
        raw[...] = dot(hidden[...], second_buf[...])
        if i + 1 < len(items):
            first_half(i + 1, 1)
        finish(i)
        if branch == 2:
            finish_cells(b)
    for b in range(blocks):
        c_out(b).wait()


def decode(sources, incoming, before, before_grid, grid, first, second, grid_first, grid_second):
    cells, width = grid.shape
    blocks = cells // CELLS
    hb = pl.BlockSpec(memory_space=HBM)
    return pl.pallas_call(
        decode_kernel,
        out_shape=jax.ShapeDtypeStruct((cells, width), bf16),
        in_specs=[pl.BlockSpec(memory_space=VMEM)] * 2 + [hb] * 7,
        out_specs=hb,
        scratch_shapes=[
            VMEM((width, width), bf16),
            VMEM((3, cells, width), bf16),
            VMEM((cells, width), bf16),
            VMEM((cells, width), bf16),
            VMEM((width, width), bf16),
            VMEM((width, width), bf16),
            VMEM((width, width), bf16),
            VMEM((incoming.shape[0] // 2, width), bf16),
            VMEM((3, CELLS, incoming.shape[0] // 2), bf16),
            VMEM((2, CELLS, width), f32),
            VMEM((CELLS, width), f32),
            VMEM((CELLS, width), bf16),
            VMEM((CELLS, width), f32),
            VMEM((CELLS, width), f32),
            VMEM((CELLS, width), bf16),
            VMEM((CELLS, width), f32),
            VMEM((cells, width), bf16),
            pltpu.SemaphoreType.DMA((5,)),
            pltpu.SemaphoreType.DMA((3, blocks)),
            pltpu.SemaphoreType.DMA((blocks,)),
        ],
        compiler_params=pltpu.CompilerParams(vmem_limit_bytes=GRANT),
        cost_estimate=pl.CostEstimate(flops=16 * cells * width * width, bytes_accessed=13 << 20, transcendentals=0),
        name="decode",
    )(sources, incoming, *pinned(before, before_grid, grid, first, second, grid_first, grid_second))


def exchange(rows):
    chunks = rows.reshape(-1, 8, rows.shape[1])
    return lax.all_to_all(chunks, ("lat", "lon"), split_axis=0, concat_axis=0, tiled=True).reshape(rows.shape)


def shards(
    mesh_nodes,
    mesh_edges,
    grid_state,
    decoder_edges,
    edge_send,
    edge_recv,
    halo_lists,
    decoder_lists,
    decoder_sources,
    edge_first,
    edge_second,
    node_first,
    node_second,
    decoder_first,
    decoder_second,
    grid_first,
    grid_second,
):
    tile_lat, tile_lon, width = grid_state.shape
    cells = tile_lat * tile_lon
    halo = halo_lists.reshape(halo_lists.shape[1:]).T
    outgoing = pick_first(halo, mesh_nodes)
    incoming = exchange(outgoing)
    send = edge_send.reshape(-1, 128)
    recv = edge_recv.reshape(-1, 128)
    decoder_rows = decoder_lists.reshape(decoder_lists.shape[1:]).T
    grid = grid_state.reshape(cells, width)
    sources = decoder_sources.reshape(-1, 128)
    nodes, edges = mesh_nodes, mesh_edges
    layers = edge_first.shape[0]
    for layer in range(layers):
        last = layer == layers - 1
        before = edges_before(edges, send, recv, nodes, edge_first, layer)
        results = run_layer(
            layer, last, send, recv, decoder_rows if last else halo, incoming, before, edges, nodes,
            edge_first, edge_second, node_first, node_second,
        )
        nodes, outgoing = results[:2]
        if not last:
            edges = results[2]
        incoming = exchange(outgoing)
    before, before_grid = decode_before(decoder_edges.reshape(3, cells, width), grid, decoder_first, grid_first)
    final = decode(
        sources, incoming, before, before_grid, grid, decoder_first, decoder_second, grid_first, grid_second
    )
    return nodes, final.reshape(tile_lat, tile_lon, width)


def solution(mesh):
    placed = (
        P(("lat", "lon"), None),
        P(("lat", "lon"), None),
        P("lat", "lon", None),
        P(None, "lat", "lon", None),
        P(("lat", "lon")),
        P(("lat", "lon")),
        P(("lat", "lon"), None, None),
        P(("lat", "lon"), None, None),
        P(None, "lat", "lon"),
        P(),
        P(),
        P(),
        P(),
        P(),
        P(),
        P(),
        P(),
    )
    return jax.shard_map(
        shards,
        mesh=mesh,
        in_specs=placed,
        out_specs=(P(("lat", "lon"), None), P("lat", "lon", None)),
        check_vma=False,
    )
```

```python
import functools

import jax
import jax.numpy as jnp
from jax import lax
from jax.experimental import pallas as pl
from jax.experimental.pallas import tpu as pltpu
from jax.sharding import PartitionSpec as P

epsilon = 1e-05
BLOCK = 512
SUB = 256
CHUNK = 32
CELLS = 256
GRANT = 40 << 20
FULL = 62 << 20
bf16 = jnp.bfloat16
f32 = jnp.float32
HBM = pltpu.HBM
VMEM = pltpu.VMEM


def pinned(*arrays):
    return [pltpu.with_memory_space_constraint(a, HBM) for a in arrays]


def dot(a, b):
    return jnp.dot(a, b, preferred_element_type=f32)


def silu_of_double(half):
    return half + half * jnp.tanh(half)


def normalize(values):
    average = jnp.mean(values, axis=-1, keepdims=True)
    centered = values - average
    spread = jnp.mean(centered * centered, axis=-1, keepdims=True)
    return centered * lax.rsqrt(spread + epsilon)


def tail(half, second):
    return normalize(dot(silu_of_double(half).astype(bf16), second))


def picker_rows(row, table_rows, first):
    spread = jnp.broadcast_to(row.astype(f32), (128, 128)).T
    lanes = lax.broadcasted_iota(jnp.int32, (128, 128), 1).astype(f32)
    shifted = spread - lanes
    pieces = [
        jnp.where(shifted == float(first + c * 128), 1.0, 0.0).astype(bf16)
        for c in range(table_rows // 128)
    ]
    return jnp.concatenate(pieces, axis=1)


def fill_picker(oh_ref, idx_ref, first_index_row, rows, table_rows, first):
    for r in range(rows // 128):
        row = idx_ref[pl.ds(first_index_row + r, 1), :]
        oh_ref[r * 128 : (r + 1) * 128, :] = picker_rows(row, table_rows, first)


def fill_lists(oh_ref, lists_ref, spread_ref):
    slots = lists_ref.shape[0]
    for s in range(8):
        row = lists_ref[s % slots : s % slots + 1, :]
        spread_ref[pl.ds(s, 128, stride=8), :] = jnp.broadcast_to(row.astype(f32), (128, 128)).T
    lanes = lax.broadcasted_iota(jnp.int32, spread_ref.shape, 1).astype(f32)
    shifted = spread_ref[...] - lanes
    for c in range(oh_ref.shape[1] // 128):
        oh_ref[:, c * 128 : (c + 1) * 128] = jnp.where(shifted == float(c * 128), 1.0, 0.0).astype(bf16)


def pick_kernel(lists, nodes, out, oh, spread):
    fill_lists(oh, lists, spread)
    out[...] = dot(oh[...], nodes[...]).astype(bf16)


def pick_first(lists, nodes):
    rows = lists.shape[1] * 8
    return pl.pallas_call(
        pick_kernel,
        out_shape=jax.ShapeDtypeStruct((rows, nodes.shape[1]), bf16),
        in_specs=[pl.BlockSpec(memory_space=VMEM)] * 2,
        out_specs=pl.BlockSpec(memory_space=VMEM),
        scratch_shapes=[VMEM((rows, nodes.shape[0]), bf16), VMEM((rows, 128), f32)],
        compiler_params=pltpu.CompilerParams(vmem_limit_bytes=FULL),
        cost_estimate=pl.CostEstimate(
            flops=2 * rows * nodes.shape[0] * nodes.shape[1], bytes_accessed=1 << 20, transcendentals=0
        ),
        name="pick_first",
    )(lists, nodes)


def before_kernel(edges, send, recv, nodes, first, out, oh):
    block = pl.program_id(0)
    width = nodes.shape[1]
    count = nodes.shape[0]

    rows = edges.shape[0]
    steps = rows // 128
    fill_picker(oh, send, block * steps, rows, count, 0)
    from_send = dot(oh[...], nodes[...]).astype(bf16)
    total = dot(edges[...], first[0, :width, :]) + dot(from_send, first[0, width : 2 * width, :])
    fill_picker(oh, recv, block * steps, rows, count, 0)
    from_recv = dot(oh[...], nodes[...]).astype(bf16)
    out[...] = (0.5 * (total + dot(from_recv, first[0, 2 * width :, :]))).astype(bf16)


def edges_before(edges, send, recv, nodes, edge_first, layer):
    count, width = edges.shape
    blocks = count // BLOCK
    clamp = lambda i: (i, 0)
    whole = lambda i: (0, 0)
    grid_spec = pl.GridSpec(
        grid=(blocks,),
        in_specs=[
            pl.BlockSpec((BLOCK, width), clamp),
            pl.BlockSpec(send.shape, whole),
            pl.BlockSpec(recv.shape, whole),
            pl.BlockSpec(nodes.shape, whole),
            pl.BlockSpec((1, 3 * width, width), lambda i: (layer, 0, 0)),
        ],
        out_specs=pl.BlockSpec((BLOCK, width), clamp),
        scratch_shapes=[VMEM((BLOCK, nodes.shape[0]), bf16)],
    )
    return pl.pallas_call(
        before_kernel,
        grid_spec=grid_spec,
        out_shape=jax.ShapeDtypeStruct((count, width), bf16),
        compiler_params=pltpu.CompilerParams(vmem_limit_bytes=GRANT),
        cost_estimate=pl.CostEstimate(flops=8 * count * width * width, bytes_accessed=8 << 20, transcendentals=0),
        name=f"edges_before_{layer}",
    )(edges, send, recv, nodes, edge_first)


def layer_kernel(
    layer,
    last,
    send,
    recv,
    lists,
    incoming,
    before,
    edges,
    nodes,
    edge_first,
    edge_second,
    node_first,
    node_second,
    *rest,
):
    if last:
        nodes_out, outgoing = rest[:2]
        rest = rest[2:]
        fresh_out = fresh = out_sem = edge_buf = None
    else:
        nodes_out, outgoing, fresh_out = rest[:3]
        rest = rest[3:]
        edge_buf, fresh, out_sem = rest[:3]
        rest = rest[3:]
    send_buf, before_buf, second_buf, node_buf, nf_buf, ns_buf, table, oh, ready, oh_lists, acc, spread, hidden, raw, message, scatter, sem, bsem = rest
    width = nodes.shape[1]
    count = nodes.shape[0]
    blocks = before.shape[0] // BLOCK

    def copy(src, dst, which):
        return pltpu.make_async_copy(src, dst, sem.at[which])

    c_send = copy(edge_first.at[layer, pl.ds(width, width), :], send_buf, 1)
    c_second = copy(edge_second.at[layer], second_buf, 2)
    c_node = copy(nodes, node_buf, 3)
    c_nf = copy(node_first.at[layer], nf_buf, 4)
    c_ns = copy(node_second.at[layer], ns_buf, 5)

    def c_before(b):
        return pltpu.make_async_copy(
            before.at[pl.ds(b * BLOCK, BLOCK), :], before_buf.at[pl.ds(b * BLOCK, BLOCK), :], bsem.at[0, b]
        )

    def c_edge(b):
        return pltpu.make_async_copy(
            edges.at[pl.ds(b * BLOCK, BLOCK), :], edge_buf.at[pl.ds(b * BLOCK, BLOCK), :], bsem.at[1, b]
        )

    def c_fresh(b):
        return pltpu.make_async_copy(
            fresh.at[pl.ds(b * BLOCK, BLOCK), :], fresh_out.at[pl.ds(b * BLOCK, BLOCK), :], out_sem.at[b]
        )

    c_send.start()
    c_before(0).start()
    c_second.start()
    for b in range(1, blocks):
        c_before(b).start()
    if not last:
        for b in range(blocks):
            c_edge(b).start()
    c_node.start()
    c_nf.start()
    c_ns.start()
    steps = SUB // 128
    items = before.shape[0] // SUB

    def picker(i):
        fill_picker(oh.at[i % 3], send, i * steps, SUB, table.shape[0], count)

    def first_half(i, part):
        columns = slice(part * (width // 2), (part + 1) * (width // 2))
        ready[i % 2, :, columns] = dot(oh[i % 3], table[:, columns])

    def hide(i):
        for c in range(0, SUB, CHUNK):
            half = ready[i % 2, c : c + CHUNK, :] + before_buf[i * SUB + c : i * SUB + c + CHUNK, :].astype(f32)
            hidden[c : c + CHUNK, :] = silu_of_double(half).astype(bf16)

    def finish(i):
        for r in range(steps):
            row = jnp.broadcast_to(recv[i * steps + r : i * steps + r + 1, :], (count, 128))
            hit = lax.broadcasted_iota(jnp.int32, (count, 128), 0) == row
            scatter[:, r * 128 : (r + 1) * 128] = jnp.where(hit, 1.0, 0.0).astype(bf16)
        for c in range(0, SUB, CHUNK):
            rows = slice(i * SUB + c, i * SUB + c + CHUNK)
            result = normalize(raw[c : c + CHUNK, :])
            message[c : c + CHUNK, :] = result.astype(bf16)
            if not last:
                fresh[rows, :] = (edge_buf[rows, :].astype(f32) + result).astype(bf16)
        part = dot(scatter[...], message[...])
        if i == 0:
            acc[...] = part
        else:
            acc[...] += part

    picker(0)
    picker(1)
    fill_lists(oh_lists, lists, spread)
    c_send.wait()
    table[...] = (0.5 * dot(incoming[...], send_buf[...])).astype(bf16)
    c_second.wait()
    per = BLOCK // SUB
    c_before(0).wait()
    first_half(0, 0)
    first_half(0, 1)
    for i in range(items):
        if i + 1 < items and (i + 1) % per == 0:
            c_before((i + 1) // per).wait()
        if not last and i % per == 0:
            c_edge(i // per).wait()
        if i + 2 < items:
            picker(i + 2)
        hide(i)
        if i + 1 < items:
            first_half(i + 1, 0)
        raw[...] = dot(hidden[...], second_buf[...])
        if i + 1 < items:
            first_half(i + 1, 1)
        finish(i)
        if not last and (i + 1) % (BLOCK // SUB) == 0:
            c_fresh(i // (BLOCK // SUB)).start()
    c_node.wait()
    c_nf.wait()
    c_ns.wait()
    now = node_buf[...]
    before_node = 0.5 * (dot(now, nf_buf[:width, :]) + dot(acc[...].astype(bf16), nf_buf[width:, :]))
    updated = (now.astype(f32) + tail(before_node, ns_buf[...])).astype(bf16)
    nodes_out[...] = updated
    picked = dot(oh_lists[...], updated)
    if last:
        half = width // 2
        place = lax.broadcasted_iota(jnp.int32, (picked.shape[0], half), 0) % 8
        picked = jnp.where(place < 4, picked[:, :half], picked[:, half:])
    outgoing[...] = picked.astype(bf16)
    if not last:
        for b in range(blocks):
            c_fresh(b).wait()


def run_layer(layer, last, send, recv, lists, incoming, before, edges, nodes, ef, es, nf, ns):
    count, width = nodes.shape
    edge_count = edges.shape[0]
    blocks = edge_count // BLOCK
    out_rows = lists.shape[1] * 8
    vm = pl.BlockSpec(memory_space=VMEM)
    hb = pl.BlockSpec(memory_space=HBM)
    out_shape = [
        jax.ShapeDtypeStruct((count, width), bf16),
        jax.ShapeDtypeStruct((out_rows, width // 2 if last else width), bf16),
    ]
    out_specs = [vm, vm]
    scratch = []
    if not last:
        out_shape.append(jax.ShapeDtypeStruct((edge_count, width), bf16))
        out_specs.append(hb)
        scratch += [VMEM((edge_count, width), bf16), VMEM((edge_count, width), bf16), pltpu.SemaphoreType.DMA((blocks,))]
    scratch += [
        VMEM((width, width), bf16),
        VMEM((edge_count, width), bf16),
        VMEM((width, width), bf16),
        VMEM((count, width), bf16),
        VMEM((2 * width, width), bf16),
        VMEM((width, width), bf16),
        VMEM(incoming.shape, bf16),
        VMEM((3, SUB, incoming.shape[0]), bf16),
        VMEM((2, SUB, width), f32),
        VMEM((out_rows, count), bf16),
        VMEM((count, width), f32),
        VMEM((out_rows, 128), f32),
        VMEM((SUB, width), bf16),
        VMEM((SUB, width), f32),
        VMEM((SUB, width), bf16),
        VMEM((count, SUB), bf16),
        pltpu.SemaphoreType.DMA((6,)),
        pltpu.SemaphoreType.DMA((2, blocks)),
    ]
    return pl.pallas_call(
        functools.partial(layer_kernel, layer, last),
        out_shape=out_shape,
        in_specs=[vm] * 4 + [hb] * 7,
        out_specs=out_specs,
        scratch_shapes=scratch,
        compiler_params=pltpu.CompilerParams(vmem_limit_bytes=GRANT),
        cost_estimate=pl.CostEstimate(flops=9 * edge_count * width * width, bytes_accessed=12 << 20, transcendentals=0),
        name=f"layer_{layer}",
    )(send, recv, lists, incoming, *pinned(before, edges, nodes, ef, es, nf, ns))


def decode_before_kernel(edges, grid, first, grid_first, out, out_grid):
    width = grid.shape[1]
    cells = grid.shape[0]
    out_grid[...] = (0.5 * dot(grid[...], grid_first[...])).astype(bf16)
    rows = edges[...].reshape(3 * cells, width)
    own = dot(rows, first[:width, :]).reshape(3, cells, width)
    out[...] = (0.5 * (own + dot(grid[...], first[2 * width :, :])[None])).astype(bf16)


def decode_before(edges, grid, first, grid_first):
    cells, width = grid.shape
    whole = lambda i: (0, 0)
    return pl.pallas_call(
        decode_before_kernel,
        grid=(cells // CELLS,),
        in_specs=[
            pl.BlockSpec((3, CELLS, width), lambda i: (0, i, 0)),
            pl.BlockSpec((CELLS, width), lambda i: (i, 0)),
            pl.BlockSpec((3 * width, width), whole),
            pl.BlockSpec((width, width), whole),
        ],
        out_specs=[
            pl.BlockSpec((3, CELLS, width), lambda i: (0, i, 0)),
            pl.BlockSpec((CELLS, width), lambda i: (i, 0)),
        ],
        out_shape=[
            jax.ShapeDtypeStruct((3, cells, width), bf16),
            jax.ShapeDtypeStruct((cells, width), bf16),
        ],
        compiler_params=pltpu.CompilerParams(vmem_limit_bytes=FULL),
        cost_estimate=pl.CostEstimate(flops=10 * cells * width * width, bytes_accessed=14 << 20, transcendentals=0),
        name="decode_before",
    )(edges, grid, first, grid_first)


def decode_kernel(
    sources, incoming, before, before_grid, grid, first, second, grid_first, grid_second, out,
    mid_buf, before_buf, bg_buf, grid_buf, second_buf, gf_buf, gs_buf, table, oh, ready, summed, hidden, raw, ready_cells, hidden_cells, raw_cells, out_buf, sem, bsem, osem,
):
    width = grid.shape[1]
    cells = grid.shape[0]
    blocks = cells // CELLS
    half = width // 2

    def copy(src, dst, which):
        return pltpu.make_async_copy(src, dst, sem.at[which])

    c_mid = copy(first.at[pl.ds(width, width), :], mid_buf, 1)
    c_second = copy(second, second_buf, 2)
    c_gf = copy(grid_first.at[pl.ds(width, width), :], gf_buf, 3)
    c_gs = copy(grid_second, gs_buf, 4)

    def c_before(b):
        rows = pl.ds(b * CELLS, CELLS)
        return pltpu.make_async_copy(before.at[:, rows, :], before_buf.at[:, rows, :], bsem.at[0, b])

    def c_bg(b):
        rows = pl.ds(b * CELLS, CELLS)
        return pltpu.make_async_copy(before_grid.at[rows, :], bg_buf.at[rows, :], bsem.at[1, b])

    def c_grid(b):
        rows = pl.ds(b * CELLS, CELLS)
        return pltpu.make_async_copy(grid.at[rows, :], grid_buf.at[rows, :], bsem.at[2, b])

    def c_out(b):
        rows = pl.ds(b * CELLS, CELLS)
        return pltpu.make_async_copy(out_buf.at[rows, :], out.at[rows, :], osem.at[b])

    c_mid.start()
    c_before(0).start()
    c_second.start()
    c_gf.start()
    c_gs.start()
    c_bg(0).start()
    c_grid(0).start()
    for b in range(1, blocks):
        c_before(b).start()
        c_bg(b).start()
        c_grid(b).start()
    packed = incoming[...].astype(f32).reshape(cells // 16, 16, half)
    even, odd = packed[:, :8, :], packed[:, 8:, :]
    low = lax.broadcasted_iota(jnp.int32, even.shape, 1) < 4
    left = jnp.where(low, even, pltpu.roll(odd, 4, 1))
    right = jnp.where(low, pltpu.roll(even, 4, 1), odd)
    left = left.reshape(cells // 2, half).astype(bf16)
    right = right.reshape(cells // 2, half).astype(bf16)
    c_mid.wait()
    table[...] = (0.5 * (dot(left, mid_buf[:half, :]) + dot(right, mid_buf[half:, :]))).astype(bf16)
    c_second.wait()
    c_before(0).wait()
    steps = CELLS // 128
    items = [(b, branch) for b in range(blocks) for branch in range(3)]

    def picker(i):
        b, branch = items[i]
        fill_picker(oh.at[i % 3], sources, branch * (cells // 128) + b * steps, CELLS, table.shape[0], 0)

    def first_half(i, part):
        columns = slice(part * half, (part + 1) * half)
        ready[i % 2, :, columns] = dot(oh[i % 3], table[:, columns])

    def hide(i):
        b, branch = items[i]
        for c in range(0, CELLS, CHUNK):
            rows = slice(b * CELLS + c, b * CELLS + c + CHUNK)
            value = ready[i % 2, c : c + CHUNK, :] + before_buf[branch, rows, :].astype(f32)
            hidden[c : c + CHUNK, :] = silu_of_double(value).astype(bf16)

    def finish(i):
        branch = items[i][1]
        for c in range(0, CELLS, CHUNK):
            rows = slice(c, c + CHUNK)
            result = normalize(raw[rows, :]).astype(bf16).astype(f32)
            summed[rows, :] = result if branch == 0 else summed[rows, :] + result

    def finish_cells(b):
        if b == 0:
            c_gf.wait()
            c_gs.wait()
        c_bg(b).wait()
        c_grid(b).wait()
        ready_cells[...] = dot(summed[...].astype(bf16), gf_buf[...])
        for c in range(0, CELLS, CHUNK):
            rows = slice(b * CELLS + c, b * CELLS + c + CHUNK)
            value = 0.5 * ready_cells[c : c + CHUNK, :] + bg_buf[rows, :].astype(f32)
            hidden_cells[c : c + CHUNK, :] = silu_of_double(value).astype(bf16)
        raw_cells[...] = dot(hidden_cells[...], gs_buf[...])
        for c in range(0, CELLS, CHUNK):
            rows = slice(b * CELLS + c, b * CELLS + c + CHUNK)
            result = normalize(raw_cells[c : c + CHUNK, :])
            out_buf[rows, :] = (grid_buf[rows, :].astype(f32) + result).astype(bf16)
        c_out(b).start()

    picker(0)
    picker(1)
    first_half(0, 0)
    first_half(0, 1)
    for i, (b, branch) in enumerate(items):
        if branch == 2 and b + 1 < blocks:
            c_before(b + 1).wait()
        if i + 2 < len(items):
            picker(i + 2)
        hide(i)
        if i + 1 < len(items):
            first_half(i + 1, 0)
        raw[...] = dot(hidden[...], second_buf[...])
        if i + 1 < len(items):
            first_half(i + 1, 1)
        finish(i)
        if branch == 2:
            finish_cells(b)
    for b in range(blocks):
        c_out(b).wait()


def decode(sources, incoming, before, before_grid, grid, first, second, grid_first, grid_second):
    cells, width = grid.shape
    blocks = cells // CELLS
    hb = pl.BlockSpec(memory_space=HBM)
    return pl.pallas_call(
        decode_kernel,
        out_shape=jax.ShapeDtypeStruct((cells, width), bf16),
        in_specs=[pl.BlockSpec(memory_space=VMEM)] * 2 + [hb] * 7,
        out_specs=hb,
        scratch_shapes=[
            VMEM((width, width), bf16),
            VMEM((3, cells, width), bf16),
            VMEM((cells, width), bf16),
            VMEM((cells, width), bf16),
            VMEM((width, width), bf16),
            VMEM((width, width), bf16),
            VMEM((width, width), bf16),
            VMEM((incoming.shape[0] // 2, width), bf16),
            VMEM((3, CELLS, incoming.shape[0] // 2), bf16),
            VMEM((2, CELLS, width), f32),
            VMEM((CELLS, width), f32),
            VMEM((CELLS, width), bf16),
            VMEM((CELLS, width), f32),
            VMEM((CELLS, width), f32),
            VMEM((CELLS, width), bf16),
            VMEM((CELLS, width), f32),
            VMEM((cells, width), bf16),
            pltpu.SemaphoreType.DMA((5,)),
            pltpu.SemaphoreType.DMA((3, blocks)),
            pltpu.SemaphoreType.DMA((blocks,)),
        ],
        compiler_params=pltpu.CompilerParams(vmem_limit_bytes=GRANT),
        cost_estimate=pl.CostEstimate(flops=16 * cells * width * width, bytes_accessed=13 << 20, transcendentals=0),
        name="decode",
    )(sources, incoming, *pinned(before, before_grid, grid, first, second, grid_first, grid_second))


def exchange(rows):
    chunks = rows.reshape(-1, 8, rows.shape[1])
    return lax.all_to_all(chunks, ("lat", "lon"), split_axis=0, concat_axis=0, tiled=True).reshape(rows.shape)


def shards(
    mesh_nodes,
    mesh_edges,
    grid_state,
    decoder_edges,
    edge_send,
    edge_recv,
    halo_lists,
    decoder_lists,
    decoder_sources,
    edge_first,
    edge_second,
    node_first,
    node_second,
    decoder_first,
    decoder_second,
    grid_first,
    grid_second,
):
    tile_lat, tile_lon, width = grid_state.shape
    cells = tile_lat * tile_lon
    halo = halo_lists.reshape(halo_lists.shape[1:]).T
    outgoing = pick_first(halo, mesh_nodes)
    incoming = exchange(outgoing)
    send = edge_send.reshape(-1, 128)
    recv = edge_recv.reshape(-1, 128)
    decoder_rows = decoder_lists.reshape(decoder_lists.shape[1:]).T
    grid = grid_state.reshape(cells, width)
    sources = decoder_sources.reshape(-1, 128)
    nodes, edges = mesh_nodes, mesh_edges
    layers = edge_first.shape[0]
    for layer in range(layers):
        last = layer == layers - 1
        before = edges_before(edges, send, recv, nodes, edge_first, layer)
        results = run_layer(
            layer, last, send, recv, decoder_rows if last else halo, incoming, before, edges, nodes,
            edge_first, edge_second, node_first, node_second,
        )
        nodes, outgoing = results[:2]
        if not last:
            edges = results[2]
        incoming = exchange(outgoing)
    before, before_grid = decode_before(decoder_edges.reshape(3, cells, width), grid, decoder_first, grid_first)
    final = decode(
        sources, incoming, before, before_grid, grid, decoder_first, decoder_second, grid_first, grid_second
    )
    return nodes, final.reshape(tile_lat, tile_lon, width)


def solution(mesh):
    placed = (
        P(("lat", "lon"), None),
        P(("lat", "lon"), None),
        P("lat", "lon", None),
        P(None, "lat", "lon", None),
        P(("lat", "lon")),
        P(("lat", "lon")),
        P(("lat", "lon"), None, None),
        P(("lat", "lon"), None, None),
        P(None, "lat", "lon"),
        P(),
        P(),
        P(),
        P(),
        P(),
        P(),
        P(),
        P(),
    )
    return jax.shard_map(
        shards,
        mesh=mesh,
        in_specs=placed,
        out_specs=(P(("lat", "lon"), None), P("lat", "lon", None)),
        check_vma=False,
    )
```
